32 devices in a mesh: dp: 8 (over y, x, core), mp: 4 (over z).
Axes of the slice: x: 2, y: 2, z: 4, core: 2. Of those that a mesh axis runs over, the one named last changes fastest.
Arguments:
- activations: bfloat16 [8192, 4096], P(('dp', 'mp')), may hold values from -17 to 17
- output_grads: bfloat16 [8192, 14336], P('dp', 'mp'), may hold values from -0.046875 to 0.046875
- q_start: float32 [14336, 64], P('mp'), may hold values from -6 to 6
Outputs:
- new_error: bfloat16 [32768, 14336], P('dp', 'mp')
- q_factor: float32 [14336, 64], P('mp')
The draws below stay inside these ranges and needn't reach their ends.
All inputs are finite; a program needn't handle non-finite values.
Results may differ from the reference program's by a relative error of at most 0.01.
Values may be sent and summed in bfloat16 or wider, within the bound.
No kernel may reach another device: no remote copies, remote signals or barrier semaphores. Data moves between devices by JAX's collectives and lax.ppermute only.
A program may use at most 192 MiB of HBM per device.

```python
import jax
import jax.numpy as jnp
from jax import lax

D = 4096
FF = 14336
R = 64
TOK_REP = 1024
TOKENS = 8192
N_DP = 8


def draw_activations(key, part):
    key_base = jax.random.fold_in(key, 11)
    key_cols = jax.random.fold_in(key, 12)
    column = jnp.arange(D, dtype=jnp.float32) / D
    ramp = jnp.exp(jnp.log(3.0) * (column - 0.5))
    rough = jnp.exp(jax.random.uniform(key_cols, (D,), jnp.float32, -1.15, 1.15))
    scales = ramp * rough / 1.3
    base = jax.random.normal(key_base, (TOKENS, D), jnp.float32)
    base = jnp.clip(base, -4.0, 4.0)
    return (base * scales[None, :]).astype(jnp.bfloat16)


def shard_levels(rng, dims, split, least, largest):
    factor_of = 1.0
    for position, shards_of in split:
        draws = jax.random.uniform(jax.random.fold_in(jax.random.fold_in(rng, 6), position), (shards_of,), jnp.float32, least / len(split), largest / len(split))
        factor_of = factor_of * jnp.repeat(jnp.exp(draws), dims[position] // shards_of).reshape((-1,) + (1,) * (len(dims) - 1 - position))
    return factor_of


def normal_values(rng, shape, width, most, pieces=(), kind=jnp.bfloat16):
    array = width * jax.random.normal(rng, shape, jnp.float32)
    if pieces:
        array = array * shard_levels(rng, shape, pieces, -0.22, 0.18)
    return jnp.clip(array, -most, most).astype(kind)


def setup_inputs(seed: int = 0) -> dict:
    seeds = jax.random.split(jax.random.key(seed), 4)
    activations = draw_activations(jax.random.fold_in(seeds[3], 71), 0)
    output_grads = normal_values(seeds[1], (TOKENS, FF), (16 * TOK_REP) ** -0.5, 0.046875, ((0, 8), (1, 4)))
    q_start = normal_values(seeds[2], (FF, R), 1.0, 6.0, ((0, 4),), jnp.float32)
    return {"activations": activations, "output_grads": output_grads, "q_start": q_start}


def reference(activations, output_grads, q_start):
    highest = lax.Precision.HIGHEST
    inputs_rep = activations.reshape(N_DP, TOK_REP, D)
    grads_rep = output_grads.reshape(N_DP, TOK_REP, FF)

    def left_step(carry, pair):
        inputs, grads = pair
        projected = jnp.dot(grads.astype(jnp.float32), q_start, precision=highest)
        return (carry + jnp.dot(inputs.astype(jnp.float32).T, projected, precision=highest), None)
    p_summed, unused = lax.scan(left_step, jnp.zeros((D, R), jnp.float32), (inputs_rep, grads_rep))
    p_mean = p_summed / N_DP
    gram_matrix = jnp.dot(p_mean.T, p_mean, precision=highest)
    lower_tri = jnp.linalg.cholesky(gram_matrix)
    p_ortho = lax.linalg.triangular_solve(lower_tri, p_mean, left_side=False, lower=True, transpose_a=True)

    def right_step(carry, pair):
        inputs, grads = pair
        gradient = jnp.dot(inputs.T.astype(jnp.float32), grads.astype(jnp.float32), preferred_element_type=jnp.float32)
        return (carry + jnp.dot(gradient.T, p_ortho, precision=highest), None)
    q_summed, unused_two = lax.scan(right_step, jnp.zeros((FF, R), jnp.float32), (inputs_rep, grads_rep))
    q_factor = q_summed / N_DP
    decompressed = jnp.dot(p_ortho, q_factor.T, precision=highest)

    def error_one(pair):
        inputs, grads = pair
        gradient = jnp.dot(inputs.T.astype(jnp.float32), grads.astype(jnp.float32), preferred_element_type=jnp.float32)
        return (gradient - decompressed).astype(jnp.bfloat16)
    errors = lax.map(error_one, (inputs_rep, grads_rep))
    return (errors.reshape(N_DP * D, FF), q_factor)
```

```python
import functools

import jax
import jax.numpy as jnp
from jax import lax
from jax.experimental import pallas as pl
from jax.experimental.pallas import tpu as pltpu
from jax.sharding import PartitionSpec as P

F32 = jnp.float32
BF16 = jnp.bfloat16
HIGHEST = lax.Precision.HIGHEST
ROWS_ROWS = (((0,), (0,)), ((), ()))
COLS_COLS = (((1,), (1,)), ((), ()))


def split_parts(values):
    upper = values.astype(BF16)
    lower = (values - upper.astype(F32)).astype(BF16)
    return upper, lower


def split_dot(left, right, dims):
    rows = left.shape[0]
    both = lax.dot_general(
        jnp.concatenate(split_parts(left), 0), right, dims, preferred_element_type=F32
    )
    return both[:rows] + both[rows:]


def ring(count, shift):
    return [(i, (i + shift) % count) for i in range(count)]


def flip(count, mask):
    return [(i, i ^ mask) for i in range(count)]


def scatter_lanes(values, axis):
    count, me = lax.axis_size(axis), lax.axis_index(axis)
    width = values.shape[1] // count

    def block(k):
        return lax.dynamic_slice_in_dim(values, lax.rem(me + k, count) * width, width, 1)

    total = block(0)
    got = [lax.ppermute(block(k), axis, ring(count, k)) for k in range(1, count)]
    for part in got:
        total = total + part
    return total


def gather_lanes(values, axis):
    count, me = lax.axis_size(axis), lax.axis_index(axis)
    rows, width = values.shape
    got = [values] + [lax.ppermute(values, axis, ring(count, k)) for k in range(1, count)]
    out = jnp.zeros((rows, count * width), values.dtype)
    for k, part in enumerate(got):
        out = lax.dynamic_update_slice_in_dim(out, part, lax.rem(me + count - k, count) * width, 1)
    return out


def scatter_rows(values, axis):
    count, me = lax.axis_size(axis), lax.axis_index(axis)
    rows, width = values.shape
    each = rows // count
    blocks = values.reshape(count // 2, 2, each, width)
    bit = lax.rem(me, 2)
    keep = lax.dynamic_index_in_dim(blocks, bit, 1, keepdims=False)
    give = lax.dynamic_index_in_dim(blocks, 1 - bit, 1, keepdims=False)
    half = keep + lax.ppermute(give, axis, flip(count, 1))
    pair = me // 2

    def block(k):
        return lax.dynamic_index_in_dim(half, pair ^ k, 0, keepdims=False)

    got = [lax.ppermute(block(k), axis, flip(count, 2 * k)) for k in range(1, count // 2)]
    total = block(0)
    for part in got:
        total = total + part
    return total


def gather_rows(values, axis):
    count, me = lax.axis_size(axis), lax.axis_index(axis)
    each, width = values.shape
    pair, bit = me // 2, lax.rem(me, 2)
    got = [values] + [lax.ppermute(values, axis, flip(count, 2 * k)) for k in range(1, count // 2)]
    mine = jnp.zeros((count // 2, each, width), values.dtype)
    for k, part in enumerate(got):
        mine = lax.dynamic_update_index_in_dim(mine, part, pair ^ k, 0)
    other = lax.ppermute(mine, axis, flip(count, 1))
    first = jnp.where(bit == 0, mine, other)
    second = jnp.where(bit == 0, other, mine)
    return jnp.stack([first, second], 1).reshape(count * each, width)


def error_kernel(x_ref, p_ref, y_ref, q_ref, *refs):
    out_ref = refs[-1]
    total = lax.dot_general(x_ref[...], y_ref[...], ROWS_ROWS, preferred_element_type=F32)
    total += lax.dot_general(p_ref[...], q_ref[...], ROWS_ROWS, preferred_element_type=F32)
    out_ref[...] = total.astype(BF16)


def error_matmul(x, p_cat, y, q_cat, out, start, features, block=256):
    tokens, columns = x.shape
    hidden = y.shape[1]
    depth = p_cat.shape[0]
    first = start // block
    in_specs = [
        pl.BlockSpec((tokens, block), lambda i: (0, i)),
        pl.BlockSpec((depth, block), lambda i: (0, first + i)),
        pl.BlockSpec((tokens, hidden), lambda i: (0, 0), pipeline_mode=pl.Buffered(1)),
        pl.BlockSpec((depth, hidden), lambda i: (0, 0), pipeline_mode=pl.Buffered(1)),
    ]
    operands = [x, p_cat, y, q_cat]
    aliases = {}
    if out is not None:
        in_specs.append(pl.BlockSpec(memory_space=pl.ANY))
        operands.append(out)
        aliases = {4: 0}
    return pl.pallas_call(
        error_kernel,
        grid=(columns // block,),
        in_specs=in_specs,
        out_specs=pl.BlockSpec((block, hidden), lambda i: (first + i, 0)),
        out_shape=jax.ShapeDtypeStruct((features, hidden), BF16),
        input_output_aliases=aliases,
        cost_estimate=pl.CostEstimate(
            flops=2 * (tokens + depth) * columns * hidden,
            bytes_accessed=2 * (columns * hidden + tokens * (columns + hidden)),
            transcendentals=0,
        ),
        compiler_params=pltpu.CompilerParams(vmem_limit_bytes=56 * 1024 * 1024),
    )(*operands)


def orthonormal_inverse(gram):
    lower_tri = jnp.linalg.cholesky(gram)
    eye = jnp.eye(gram.shape[0], dtype=gram.dtype)
    return lax.linalg.triangular_solve(lower_tri, eye, left_side=True, lower=True)


def pieces(features):
    unit = features // 16
    starts = [0, 5 * unit, 10 * unit, 14 * unit, features]
    return list(zip(starts[:-1], starts[1:]))


def per_device(activations, output_grads, q_start):
    replicas = lax.axis_size("dp")
    features = activations.shape[1]
    cuts = pieces(features)
    gathered = [
        lax.all_gather(activations[:, lo:hi], "mp", axis=0, tiled=True) for lo, hi in cuts
    ]

    z_part = split_dot(q_start.T, output_grads, COLS_COLS)
    z_mine = scatter_lanes(z_part, "mp")
    p_part = split_dot(z_mine, activations, (((1,), (0,)), ((), ())))
    p_rows = scatter_rows(p_part, "dp")
    p_rows = gather_lanes(scatter_lanes(p_rows, "mp"), "mp")
    p_mean = gather_rows(p_rows, "dp") / replicas

    w_mine = split_dot(p_mean, activations, COLS_COLS)
    w_all = gather_lanes(w_mine, "mp")
    q_part = split_dot(w_all, output_grads, (((1,), (0,)), ((), ())))
    q_sum = lax.all_gather(scatter_rows(q_part, "dp"), "dp", axis=0, tiled=True) / replicas

    gram = lax.dot_general(p_mean, p_mean, COLS_COLS, precision=HIGHEST)
    inverse = orthonormal_inverse(gram)
    p_ortho = jnp.dot(inverse, p_mean, precision=HIGHEST)
    q_factor = jnp.dot(inverse, q_sum, precision=HIGHEST)

    p_up, p_low = split_parts(-p_ortho)
    q_up, q_low = split_parts(q_factor)
    p_cat = jnp.concatenate([p_up, p_up, p_low, p_low], 0)
    q_cat = jnp.concatenate([q_up, q_low, q_up, q_low], 0)
    new_error = None
    for (lo, _), x in zip(cuts, gathered):
        new_error = error_matmul(x, p_cat, output_grads, q_cat, new_error, lo, features)
    return new_error, q_factor.T


def solution(mesh):
    in_specs = (P(("dp", "mp"), None), P("dp", "mp"), P("mp", None))
    out_specs = (P("dp", "mp"), P("mp", None))
    return jax.shard_map(
        per_device, mesh=mesh, in_specs=in_specs, out_specs=out_specs, check_vma=False
    )
```
